16 devices in a mesh: dp: 2 (over y, z), sp: 8 (over x, core).
Axes of the slice: x: 4, y: 2, z: 1, core: 2. Of those that a mesh axis runs over, the one named last changes fastest.
The devices are a block of a 4x4x8 slice.
Arguments:
- signal: bfloat16 [131072, 1024], P(('dp', 'sp')), parts along dimension 0
- w_first: bfloat16 [11, 2048, 2, 32, 32], P(None, 'sp')
- w_second: bfloat16 [11, 2048, 2, 32, 32], P(None, 'sp')
Outputs:
- output: bfloat16 [131072, 1024], P(('dp', 'sp')), parts along dimension 0
There are 2 independent parts. The reference program is written for one: setup_inputs(seed, part) draws one part's arguments, and reference() takes and returns one part's arrays. A program takes and returns all parts, laid end to end along the dimension named above; an argument that names none is the same for every part.
All inputs are finite; a program needn't handle non-finite values.
Results may differ from the reference program's by a relative error of at most 0.02.
Values are sent between devices in bfloat16 or wider.
A program may use at most 768 MiB of HBM per device.

```python
import jax
import jax.numpy as jnp
import math
from jax import lax

SEQ_LEN = 65536
CHANNELS = 1024
BLOCK_SIZE = 32

NUM_BLOCKS = SEQ_LEN // BLOCK_SIZE
STAGES = int(math.log2(NUM_BLOCKS))


def setup_inputs(seed: int = 0, part: int = 0) -> dict:
    key_signal = jax.random.fold_in(jax.random.key(seed + 1), part)
    key_first = jax.random.key(seed + 2)
    key_second = jax.random.key(seed + 3)
    w_shape = (STAGES, NUM_BLOCKS, 2, BLOCK_SIZE, BLOCK_SIZE)
    w_scale = (2 * BLOCK_SIZE) ** -0.5
    signal = jax.random.normal(key_signal, (SEQ_LEN, CHANNELS), jnp.float32)
    w_first = jax.random.normal(key_first, w_shape, jnp.float32) * w_scale
    w_second = jax.random.normal(key_second, w_shape, jnp.float32) * w_scale
    return {"signal": signal.astype(jnp.bfloat16), "w_first": w_first.astype(jnp.bfloat16), "w_second": w_second.astype(jnp.bfloat16)}


def butterfly_stage(act_blocks, weights, distance):
    grouped = act_blocks.reshape(NUM_BLOCKS // (2 * distance), 2, distance, BLOCK_SIZE, act_blocks.shape[2])
    partner = grouped[:, ::-1].reshape(act_blocks.shape)
    paired = jnp.stack([act_blocks, partner], axis=1).astype(jnp.float32)
    mixed = jnp.einsum("ltij,ltjc->lic", weights.astype(jnp.float32), paired)
    return mixed.astype(jnp.bfloat16)


def apply_map(act_blocks, weights, distances):
    for stage, distance in enumerate(distances):
        act_blocks = butterfly_stage(act_blocks, weights[stage], distance)
    return act_blocks


def reference(signal, w_first, w_second):
    col_width = min(CHANNELS, 128)
    col_groups = CHANNELS // col_width
    grouped = signal.reshape(NUM_BLOCKS, BLOCK_SIZE, col_groups, col_width).transpose(2, 0, 1, 3)
    dist_down = [2 ** (STAGES - 1 - level) for level in range(STAGES)]
    dist_up = [2 ** level for level in range(STAGES)]

    def one_group(act_blocks):
        hidden = apply_map(act_blocks, w_first, dist_down)
        hidden = jax.nn.gelu(hidden.astype(jnp.float32), approximate=False).astype(jnp.bfloat16)
        return apply_map(hidden, w_second, dist_up)

    mapped = lax.map(one_group, grouped)
    return mapped.transpose(1, 2, 0, 3).reshape(SEQ_LEN, CHANNELS)
```

```python
import functools

import jax
import jax.numpy as jnp
from jax import lax
from jax.experimental import pallas as pl
from jax.experimental.pallas import tpu as pltpu
from jax.sharding import PartitionSpec as P


CORES = 2
CHIPS = 4
LANES = 128
BF16 = jnp.bfloat16
F32 = jnp.float32


def mxu(lhs, rhs):
    return jnp.dot(lhs, rhs, preferred_element_type=F32)


def cost(us):
    return pl.CostEstimate(flops=int(us * 1e8), bytes_accessed=int(us * 1e5), transcendentals=0)


def params():
    return pltpu.CompilerParams(dimension_semantics=("arbitrary",), vmem_limit_bytes=60 * 2**20)


def turned(refs, i, sel):
    wide = jnp.concatenate([ref[0, slot, i] for ref in refs for slot in range(2)], axis=0)
    return lax.dot_general(wide, sel, (((0,), (0,)), ((), ())), preferred_element_type=F32)


def pack_kernel(a_ref, b_ref, out_ref, tmp):
    blk, blocks = a_ref.shape[2], a_ref.shape[4]
    row = lax.broadcasted_iota(jnp.int32, (LANES, LANES), 0)
    col = lax.broadcasted_iota(jnp.int32, (LANES, LANES), 1)
    sel = (row == col).astype(F32).astype(BF16)

    @pl.loop(0, blk // 4)
    def _(it):
        for u in range(4):
            i = it * 4 + u
            tmp[pl.ds(i, blocks, stride=blk), :] = turned((a_ref, b_ref), i, sel)

    out_ref[...] = tmp[...].astype(BF16)


def pack_pair(turned_w, hi, lo):
    _, two, blk, _, blocks = turned_w.shape
    spec = lambda stage: pl.BlockSpec((1, two, blk, blk, blocks), lambda i: (stage, 0, 0, 0, 0))
    return pl.pallas_call(
        pack_kernel,
        grid=(1,),
        in_specs=[spec(hi), spec(lo)],
        out_specs=pl.BlockSpec((blocks * blk, LANES), lambda i: (0, 0)),
        out_shape=jax.ShapeDtypeStruct((blocks * blk, LANES), BF16),
        scratch_shapes=[pltpu.VMEM((blocks * blk, LANES), F32)],
        compiler_params=params(),
        cost_estimate=cost(5),
        name="pack_pair",
    )(turned_w, turned_w)


def expand_kernel(d0, d1, d2, d3, sel_hi, sel_lo, out_hi, out_lo):
    for rel, src in enumerate((d0, d1, d2, d3)):
        val = src[...]
        out_hi[rel] = mxu(val, sel_hi[rel]).astype(BF16)
        out_lo[rel] = mxu(val, sel_lo[rel]).astype(BF16)


def expand_pair(packed, odd, blk):
    rows = packed[0].shape[0]
    tile = rows // 8
    shape = (CHIPS, LANES, LANES)
    rel, k, n = (lax.broadcasted_iota(jnp.int32, shape, axis) for axis in range(3))
    same = k % blk == n % blk
    kg, ng = k // blk, n // blk
    mate_lo = jnp.where(odd == 1, 3 - rel, rel ^ 1)
    sel_hi = (same & (((kg == 0) & (ng == rel)) | ((kg == 1) & (ng == (rel ^ 2))))).astype(BF16)
    sel_lo = (same & (((kg == 2) & (ng == rel)) | ((kg == 3) & (ng == mate_lo)))).astype(BF16)
    out = jax.ShapeDtypeStruct((CHIPS, rows, LANES), BF16)
    sel_spec = pl.BlockSpec(shape, lambda i: (0, 0, 0))
    out_spec = pl.BlockSpec((CHIPS, tile, LANES), lambda i: (0, i, 0))
    return pl.pallas_call(
        expand_kernel,
        grid=(rows // tile,),
        in_specs=[pl.BlockSpec((tile, LANES), lambda i: (i, 0))] * 4 + [sel_spec] * 2,
        out_specs=[out_spec] * 2,
        out_shape=[out] * 2,
        compiler_params=params(),
        cost_estimate=cost(5),
        name="expand_pair",
    )(*packed, sel_hi, sel_lo)


def spread_kernel(first_map, a_ref, b_ref, out_ref, tmp_a, tmp_b):
    step = pl.program_id(0)
    blk, blocks = a_ref.shape[2], a_ref.shape[4]
    lone = step == 4
    lo = jnp.where(lone, 0, 6 - 2 * step if first_map else 2 * step)
    row = lax.broadcasted_iota(jnp.int32, (LANES, 4 * LANES), 0)
    col = lax.broadcasted_iota(jnp.int32, (LANES, 4 * LANES), 1)
    fits = row % blk == col % blk
    sel = (fits & (row // blk == col // LANES)).astype(F32).astype(BF16)
    block = lax.broadcasted_iota(jnp.int32, (blocks, LANES), 0)
    group = lax.broadcasted_iota(jnp.int32, (blocks, LANES), 1) // blk
    own = jnp.where(lone, 2 * (block & 1), (block >> lo) & 3)
    first, second = (2, 1) if first_map else (1, 2)
    mates = [jnp.where(lone, own + 1, own ^ first), jnp.where(lone, own + 1, own ^ second)]

    @pl.loop(0, blk // 8)
    def _(it):
        wides = [turned((a_ref, b_ref), it * 8 + u, sel) for u in range(8)]
        for u, wide in enumerate(wides):
            for half, (mate, tmp) in enumerate(zip(mates, (tmp_a, tmp_b))):
                both = wide[:, 2 * half * LANES : 2 * (half + 1) * LANES]
                val = jnp.where(group == own, both[:, :LANES], jnp.where(group == mate, both[:, LANES:], 0.0))
                tmp[pl.ds(it * 8 + u, blocks, stride=blk), :] = val

    out_ref[0] = tmp_a[...].astype(BF16)
    out_ref[1] = tmp_b[...].astype(BF16)


def spread(turned_w, first_map):
    stages, two, blk, _, blocks = turned_w.shape
    if first_map:
        a_at = lambda i: jnp.where(i < 4, 3 + 2 * i, 2)
        b_at = lambda i: jnp.where(i < 4, 4 + 2 * i, 2)
    else:
        a_at = lambda i: 2 * i
        b_at = lambda i: jnp.minimum(2 * i + 1, stages - 3)
    spec = lambda at: pl.BlockSpec((1, two, blk, blk, blocks), lambda i: (at(i), 0, 0, 0, 0))
    rows = blocks * blk
    return pl.pallas_call(
        functools.partial(spread_kernel, first_map),
        grid=(5,),
        in_specs=[spec(a_at), spec(b_at)],
        out_specs=pl.BlockSpec((2, rows, LANES), lambda i: (i, 0, 0)),
        out_shape=jax.ShapeDtypeStruct((10, rows, LANES), BF16),
        scratch_shapes=[pltpu.VMEM((rows, LANES), F32)] * 2,
        compiler_params=params(),
        cost_estimate=cost(25),
        name="spread",
    )(turned_w, turned_w)


def two_stages(quads):
    mids = [mxu(lhs_a, rows).astype(BF16) for lhs_a, _, rows in quads]
    return [mxu(lhs_b, mid).astype(BF16) for (_, lhs_b, _), mid in zip(quads, mids)]


def chip_kernel(blk, x0, x1, x2, x3, ea, eb, o0, o1, o2, o3):
    spans = [slice(b * blk, (b + 1) * blk) for b in range(x0.shape[0] // blk)]
    quads = []
    for rows in spans:
        z = jnp.concatenate([x[rows, :] for x in (x0, x1, x2, x3)], axis=0)
        a_mat = jnp.concatenate([ea[r, rows, :] for r in range(CHIPS)], axis=0)
        b_mat = jnp.concatenate([eb[r, rows, :] for r in range(CHIPS)], axis=0)
        quads.append((a_mat, b_mat, z))
    for rows, y in zip(spans, two_stages(quads)):
        for r, o in enumerate((o0, o1, o2, o3)):
            o[rows, :] = y[r * blk : (r + 1) * blk]


def chip_stages(parts, ea, eb, blk):
    rows, width = parts[0].shape
    tile = rows // 8
    spec = pl.BlockSpec((tile, width), lambda i: (i, 0))
    wspec = pl.BlockSpec((CHIPS, tile, LANES), lambda i: (0, i, 0))
    return pl.pallas_call(
        functools.partial(chip_kernel, blk),
        grid=(rows // tile,),
        in_specs=[spec] * 4 + [wspec] * 2,
        out_specs=[spec] * 4,
        out_shape=[jax.ShapeDtypeStruct((rows, width), BF16)] * 4,
        compiler_params=params(),
        cost_estimate=cost(8),
        name="chip_stages",
    )(*parts, ea, eb)


def gelu(x):
    x = x.astype(F32)
    return (0.5 * x * (1.0 + lax.erf(x * 0.7071067811865476))).astype(BF16)


def middle_kernel(blk, chip_ref, x0, x1, x2, x3, p0, p1, p2, p3, core_w, first_w, second_w, buf):
    step = pl.program_id(0)
    group_rows = x0.shape[0]
    unroll = 8

    @pl.when(step == 0)
    def _():
        for rel, (own, mate) in enumerate(zip((x0, x1, x2, x3), (p0, p1, p2, p3))):
            base = ((chip_ref[0] + rel) % CHIPS) * group_rows

            @pl.loop(0, group_rows // (2 * blk * unroll))
            def _(it):
                outs = []
                for u in range(unroll):
                    off = pl.multiple_of((it * unroll + u) * 2 * blk, 2 * blk)
                    nxt = pl.multiple_of(off + blk, blk)
                    dst = pl.multiple_of(base + off, 2 * blk)
                    z = jnp.concatenate(
                        [own[pl.ds(off, blk), :], mate[pl.ds(off, blk), :], own[pl.ds(nxt, blk), :], mate[pl.ds(nxt, blk), :]], axis=0
                    )
                    outs.append((dst, mxu(core_w[0, pl.ds(dst, 2 * blk), :], z).astype(BF16)))
                for dst, val in outs:
                    buf[pl.ds(dst, 2 * blk), :] = val

    def quad_step(wts, lo):
        @pl.loop(0, buf.shape[0] // (4 * blk * unroll))
        def _(it):
            places, quads = [], []
            for u in range(unroll):
                quad = it * unroll + u
                first = ((quad >> lo) << (lo + 2)) | (quad & ((1 << lo) - 1))
                offs = [pl.multiple_of((first + (pos << lo)) * blk, blk) for pos in range(4)]
                z = jnp.concatenate([buf[pl.ds(o, blk), :] for o in offs], axis=0)
                a_mat = jnp.concatenate([wts[0, pl.ds(o, blk), :] for o in offs], axis=0)
                b_mat = jnp.concatenate([wts[1, pl.ds(o, blk), :] for o in offs], axis=0)
                places.append(offs)
                quads.append((a_mat, b_mat, z))
            for offs, y in zip(places, two_stages(quads)):
                for pos, o in enumerate(offs):
                    buf[pl.ds(o, blk), :] = y[pos * blk : (pos + 1) * blk]

    @pl.when((step > 0) & (step <= 4))
    def _():
        quad_step(first_w, 8 - 2 * step)

    @pl.when(step == 4)
    def _():
        rows = 64

        @pl.loop(0, buf.shape[0] // rows)
        def _(it):
            at = pl.ds(pl.multiple_of(it * rows, rows), rows)
            buf[at, :] = gelu(buf[at, :])

    @pl.when(step > 4)
    def _():
        quad_step(second_w, 2 * step - 10)


def middle(chip, parts, mates, first_w, second_w, blk):
    rows, width = parts[0].shape
    total = rows * CHIPS
    once = pl.Buffered(1)
    full = pl.BlockSpec((rows, width), lambda i, c: (0, 0), pipeline_mode=once)
    return pl.pallas_call(
        functools.partial(middle_kernel, blk),
        grid_spec=pltpu.PrefetchScalarGridSpec(
            num_scalar_prefetch=1,
            grid=(9,),
            in_specs=[full] * 8
            + [
                pl.BlockSpec((1, total, LANES), lambda i, c: (8, 0, 0), pipeline_mode=once),
                pl.BlockSpec((2, total, LANES), lambda i, c: (jnp.clip(i - 1, 0, 3), 0, 0)),
                pl.BlockSpec((2, total, LANES), lambda i, c: (jnp.clip(i - 5, 0, 3), 0, 0)),
            ],
            out_specs=pl.BlockSpec((total, width), lambda i, c: (0, 0), pipeline_mode=once),
        ),
        out_shape=jax.ShapeDtypeStruct((total, width), BF16),
        compiler_params=params(),
        cost_estimate=cost(35),
        name="middle",
    )(chip, *parts, *mates, first_w, first_w, second_w)


def core_kernel(blk, chip_ref, *refs):
    own, mate, wts, outs = refs[0:4], refs[4:8], refs[8:12], refs[12:16]
    for rel in range(CHIPS):
        for pair in range(own[rel].shape[0] // (2 * blk)):
            at, nxt = pair * 2 * blk, pair * 2 * blk + blk
            z = jnp.concatenate(
                [own[rel][at:nxt, :], mate[rel][at:nxt, :], own[rel][nxt : nxt + blk, :], mate[rel][nxt : nxt + blk, :]], axis=0
            )
            outs[rel][at : at + 2 * blk, :] = mxu(wts[rel][0, at : at + 2 * blk, :], z).astype(BF16)


def core_stage(chip, own, mate, core_w, blk):
    total, width = own.shape
    rows = total // CHIPS
    tile = rows // 8

    def rel_spec(rel):
        return pl.BlockSpec((tile, width), lambda i, c: (((c[0] + rel) % CHIPS) * 8 + i, 0))

    def w_spec(rel):
        return pl.BlockSpec((1, tile, LANES), lambda i, c: (8, ((c[0] + rel) % CHIPS) * 8 + i, 0))

    data = [rel_spec(r) for r in range(CHIPS)]
    return pl.pallas_call(
        functools.partial(core_kernel, blk),
        grid_spec=pltpu.PrefetchScalarGridSpec(
            num_scalar_prefetch=1,
            grid=(8,),
            in_specs=data + data + [w_spec(r) for r in range(CHIPS)],
            out_specs=[pl.BlockSpec((tile, width), lambda i, c: (i, 0))] * 4,
        ),
        out_shape=[jax.ShapeDtypeStruct((rows, width), BF16)] * 4,
        compiler_params=params(),
        cost_estimate=cost(8),
        name="core_stage",
    )(chip, *[own] * 4, *[mate] * 4, *[core_w] * 4)


def solution(mesh):
    members = mesh.shape["sp"]

    def to_chip(value, shift):
        pairs = [(d, (d + shift * CORES) % members) for d in range(members)]
        return lax.ppermute(value, "sp", pairs)

    def to_core(value):
        return lax.ppermute(value, "sp", [(d, d ^ 1) for d in range(members)])

    def swap(parts):
        got = [parts[0]] + [None] * (CHIPS - 1)
        for shift in (2, 1, 3):
            got[-shift % CHIPS] = to_chip(parts[shift], shift)
        return got

    def device_program(signal, w_first, w_second):
        stages, _, _, blk, _ = w_first.shape
        rows, channels = signal.shape
        group = rows // CHIPS
        width = 256
        chunks = channels // width
        chip = lax.axis_index("sp") // CORES
        odd = chip % 2
        chip_arr = jnp.full((1,), chip, jnp.int32)

        def quarter(array, rel, col, wide):
            return lax.dynamic_slice(array, (((chip + rel) % CHIPS) * group, col), (group, wide))

        def chip_weights(weights, hi, lo):
            packed = pack_pair(weights, hi, lo)
            got = swap([quarter(packed, r, 0, LANES) for r in range(CHIPS)])
            return expand_pair(got, odd, blk)

        w_first, w_second = (jnp.transpose(w, (0, 2, 3, 4, 1)) for w in (w_first, w_second))
        hi_first, lo_first = chip_weights(w_first, 0, 1)
        mid_first = spread(w_first, True)
        mid_second = spread(w_second, False)
        hi_second, lo_second = chip_weights(w_second, stages - 1, stages - 2)

        result = jnp.zeros((rows, channels), BF16)
        for c in range(chunks):
            parts = [quarter(signal, r, c * width, width) for r in range(CHIPS)]
            signal, parts = lax.optimization_barrier((signal, parts))
            parts = swap(parts)
            parts = chip_stages(parts, hi_first, lo_first, blk)
            parts = swap(parts)
            mates = [to_core(p) for p in parts]
            act = middle(chip_arr, parts, mates, mid_first, mid_second, blk)
            twin = to_core(act)
            parts = core_stage(chip_arr, act, twin, mid_second, blk)
            parts = swap(parts)
            parts = chip_stages(parts, lo_second, hi_second, blk)
            parts = swap(parts)
            for r in range(CHIPS):
                at = (((chip + r) % CHIPS) * group, c * width)
                result = lax.dynamic_update_slice(result, parts[r], at)
        return result

    row_spec = P(("dp", "sp"), None)
    weight_spec = P(None, "sp", None, None, None)
    return jax.shard_map(device_program, mesh=mesh, in_specs=(row_spec, weight_spec, weight_spec), out_specs=row_spec, check_vma=False)
```

```python
import functools

import jax
import jax.numpy as jnp
from jax import lax
from jax.experimental import pallas as pl
from jax.experimental.pallas import tpu as pltpu
from jax.sharding import PartitionSpec as P


CORES = 2
CHIPS = 4
LANES = 128
BF16 = jnp.bfloat16
F32 = jnp.float32


def mxu(lhs, rhs):
    return jnp.dot(lhs, rhs, preferred_element_type=F32)


def cost(us):
    return pl.CostEstimate(flops=int(us * 1e8), bytes_accessed=int(us * 1e5), transcendentals=0)


def params():
    return pltpu.CompilerParams(dimension_semantics=("arbitrary",), vmem_limit_bytes=60 * 2**20)


def turned(refs, i, sel):
    wide = jnp.concatenate([ref[0, slot, i] for ref in refs for slot in range(2)], axis=0)
    return lax.dot_general(wide, sel, (((0,), (0,)), ((), ())), preferred_element_type=F32)


def pack_kernel(a_ref, b_ref, out_ref, tmp):
    blk, blocks = a_ref.shape[2], a_ref.shape[4]
    row = lax.broadcasted_iota(jnp.int32, (LANES, LANES), 0)
    col = lax.broadcasted_iota(jnp.int32, (LANES, LANES), 1)
    sel = (row == col).astype(F32).astype(BF16)

    @pl.loop(0, blk // 4)
    def _(it):
        for u in range(4):
            i = it * 4 + u
            tmp[pl.ds(i, blocks, stride=blk), :] = turned((a_ref, b_ref), i, sel)

    out_ref[...] = tmp[...].astype(BF16)


def pack_pair(turned_w, hi, lo):
    _, two, blk, _, blocks = turned_w.shape
    spec = lambda stage: pl.BlockSpec((1, two, blk, blk, blocks), lambda i: (stage, 0, 0, 0, 0))
    return pl.pallas_call(
        pack_kernel,
        grid=(1,),
        in_specs=[spec(hi), spec(lo)],
        out_specs=pl.BlockSpec((blocks * blk, LANES), lambda i: (0, 0)),
        out_shape=jax.ShapeDtypeStruct((blocks * blk, LANES), BF16),
        scratch_shapes=[pltpu.VMEM((blocks * blk, LANES), F32)],
        compiler_params=params(),
        cost_estimate=cost(5),
        name="pack_pair",
    )(turned_w, turned_w)


def expand_kernel(d0, d1, d2, d3, sel_hi, sel_lo, out_hi, out_lo):
    for rel, src in enumerate((d0, d1, d2, d3)):
        val = src[...]
        out_hi[rel] = mxu(val, sel_hi[rel]).astype(BF16)
        out_lo[rel] = mxu(val, sel_lo[rel]).astype(BF16)


def expand_pair(packed, odd, blk):
    rows = packed[0].shape[0]
    tile = rows // 8
    shape = (CHIPS, LANES, LANES)
    rel, k, n = (lax.broadcasted_iota(jnp.int32, shape, axis) for axis in range(3))
    same = k % blk == n % blk
    kg, ng = k // blk, n // blk
    mate_lo = jnp.where(odd == 1, 3 - rel, rel ^ 1)
    sel_hi = (same & (((kg == 0) & (ng == rel)) | ((kg == 1) & (ng == (rel ^ 2))))).astype(BF16)
    sel_lo = (same & (((kg == 2) & (ng == rel)) | ((kg == 3) & (ng == mate_lo)))).astype(BF16)
    out = jax.ShapeDtypeStruct((CHIPS, rows, LANES), BF16)
    sel_spec = pl.BlockSpec(shape, lambda i: (0, 0, 0))
    out_spec = pl.BlockSpec((CHIPS, tile, LANES), lambda i: (0, i, 0))
    return pl.pallas_call(
        expand_kernel,
        grid=(rows // tile,),
        in_specs=[pl.BlockSpec((tile, LANES), lambda i: (i, 0))] * 4 + [sel_spec] * 2,
        out_specs=[out_spec] * 2,
        out_shape=[out] * 2,
        compiler_params=params(),
        cost_estimate=cost(5),
        name="expand_pair",
    )(*packed, sel_hi, sel_lo)


def spread_kernel(first_map, a_ref, b_ref, out_ref, tmp_a, tmp_b):
    step = pl.program_id(0)
    blk, blocks = a_ref.shape[2], a_ref.shape[4]
    lone = step == 4
    lo = jnp.where(lone, 0, 6 - 2 * step if first_map else 2 * step)
    row = lax.broadcasted_iota(jnp.int32, (LANES, 4 * LANES), 0)
    col = lax.broadcasted_iota(jnp.int32, (LANES, 4 * LANES), 1)
    fits = row % blk == col % blk
    sel = (fits & (row // blk == col // LANES)).astype(F32).astype(BF16)
    block = lax.broadcasted_iota(jnp.int32, (blocks, LANES), 0)
    group = lax.broadcasted_iota(jnp.int32, (blocks, LANES), 1) // blk
    own = jnp.where(lone, 2 * (block & 1), (block >> lo) & 3)
    first, second = (2, 1) if first_map else (1, 2)
    mates = [jnp.where(lone, own + 1, own ^ first), jnp.where(lone, own + 1, own ^ second)]

    @pl.loop(0, blk // 8)
    def _(it):
        wides = [turned((a_ref, b_ref), it * 8 + u, sel) for u in range(8)]
        for u, wide in enumerate(wides):
            for half, (mate, tmp) in enumerate(zip(mates, (tmp_a, tmp_b))):
                both = wide[:, 2 * half * LANES : 2 * (half + 1) * LANES]
                val = jnp.where(group == own, both[:, :LANES], jnp.where(group == mate, both[:, LANES:], 0.0))
                tmp[pl.ds(it * 8 + u, blocks, stride=blk), :] = val

    out_ref[0] = tmp_a[...].astype(BF16)
    out_ref[1] = tmp_b[...].astype(BF16)


def spread(turned_w, first_map):
    stages, two, blk, _, blocks = turned_w.shape
    if first_map:
        a_at = lambda i: jnp.where(i < 4, 3 + 2 * i, 2)
        b_at = lambda i: jnp.where(i < 4, 4 + 2 * i, 2)
    else:
        a_at = lambda i: 2 * i
        b_at = lambda i: jnp.minimum(2 * i + 1, stages - 3)
    spec = lambda at: pl.BlockSpec((1, two, blk, blk, blocks), lambda i: (at(i), 0, 0, 0, 0))
    rows = blocks * blk
    return pl.pallas_call(
        functools.partial(spread_kernel, first_map),
        grid=(5,),
        in_specs=[spec(a_at), spec(b_at)],
        out_specs=pl.BlockSpec((2, rows, LANES), lambda i: (i, 0, 0)),
        out_shape=jax.ShapeDtypeStruct((10, rows, LANES), BF16),
        scratch_shapes=[pltpu.VMEM((rows, LANES), F32)] * 2,
        compiler_params=params(),
        cost_estimate=cost(25),
        name="spread",
    )(turned_w, turned_w)


def two_stages(quads):
    mids = [mxu(lhs_a, rows).astype(BF16) for lhs_a, _, rows in quads]
    return [mxu(lhs_b, mid).astype(BF16) for (_, lhs_b, _), mid in zip(quads, mids)]


def chip_kernel(blk, x0, x1, x2, x3, ea, eb, o0, o1, o2, o3):
    spans = [slice(b * blk, (b + 1) * blk) for b in range(x0.shape[0] // blk)]
    quads = []
    for rows in spans:
        z = jnp.concatenate([x[rows, :] for x in (x0, x1, x2, x3)], axis=0)
        a_mat = jnp.concatenate([ea[r, rows, :] for r in range(CHIPS)], axis=0)
        b_mat = jnp.concatenate([eb[r, rows, :] for r in range(CHIPS)], axis=0)
        quads.append((a_mat, b_mat, z))
    for rows, y in zip(spans, two_stages(quads)):
        for r, o in enumerate((o0, o1, o2, o3)):
            o[rows, :] = y[r * blk : (r + 1) * blk]


def chip_stages(parts, ea, eb, blk):
    rows, width = parts[0].shape
    tile = rows // 8
    spec = pl.BlockSpec((tile, width), lambda i: (i, 0))
    wspec = pl.BlockSpec((CHIPS, tile, LANES), lambda i: (0, i, 0))
    return pl.pallas_call(
        functools.partial(chip_kernel, blk),
        grid=(rows // tile,),
        in_specs=[spec] * 4 + [wspec] * 2,
        out_specs=[spec] * 4,
        out_shape=[jax.ShapeDtypeStruct((rows, width), BF16)] * 4,
        compiler_params=params(),
        cost_estimate=cost(8),
        name="chip_stages",
    )(*parts, ea, eb)


def gelu(x):
    x = x.astype(F32)
    return (0.5 * x * (1.0 + lax.erf(x * 0.7071067811865476))).astype(BF16)


def middle_kernel(blk, chip_ref, x0, x1, x2, x3, p0, p1, p2, p3, core_w, first_w, second_w, buf):
    step = pl.program_id(0)
    group_rows = x0.shape[0]
    unroll = 8

    @pl.when(step == 0)
    def _():
        for rel, (own, mate) in enumerate(zip((x0, x1, x2, x3), (p0, p1, p2, p3))):
            base = ((chip_ref[0] + rel) % CHIPS) * group_rows

            @pl.loop(0, group_rows // (2 * blk * unroll))
            def _(it):
                outs = []
                for u in range(unroll):
                    off = pl.multiple_of((it * unroll + u) * 2 * blk, 2 * blk)
                    nxt = pl.multiple_of(off + blk, blk)
                    dst = pl.multiple_of(base + off, 2 * blk)
                    z = jnp.concatenate(
                        [own[pl.ds(off, blk), :], mate[pl.ds(off, blk), :], own[pl.ds(nxt, blk), :], mate[pl.ds(nxt, blk), :]], axis=0
                    )
                    outs.append((dst, mxu(core_w[0, pl.ds(dst, 2 * blk), :], z).astype(BF16)))
                for dst, val in outs:
                    buf[pl.ds(dst, 2 * blk), :] = val

    def quad_step(wts, lo):
        @pl.loop(0, buf.shape[0] // (4 * blk * unroll))
        def _(it):
            places, quads = [], []
            for u in range(unroll):
                quad = it * unroll + u
                first = ((quad >> lo) << (lo + 2)) | (quad & ((1 << lo) - 1))
                offs = [pl.multiple_of((first + (pos << lo)) * blk, blk) for pos in range(4)]
                z = jnp.concatenate([buf[pl.ds(o, blk), :] for o in offs], axis=0)
                a_mat = jnp.concatenate([wts[0, pl.ds(o, blk), :] for o in offs], axis=0)
                b_mat = jnp.concatenate([wts[1, pl.ds(o, blk), :] for o in offs], axis=0)
                places.append(offs)
                quads.append((a_mat, b_mat, z))
            for offs, y in zip(places, two_stages(quads)):
                for pos, o in enumerate(offs):
                    buf[pl.ds(o, blk), :] = y[pos * blk : (pos + 1) * blk]

    @pl.when((step > 0) & (step <= 4))
    def _():
        quad_step(first_w, 8 - 2 * step)

    @pl.when(step == 4)
    def _():
        rows = 64

        @pl.loop(0, buf.shape[0] // rows)
        def _(it):
            at = pl.ds(pl.multiple_of(it * rows, rows), rows)
            buf[at, :] = gelu(buf[at, :])

    @pl.when(step > 4)
    def _():
        quad_step(second_w, 2 * step - 10)


def middle(chip, parts, mates, first_w, second_w, blk):
    rows, width = parts[0].shape
    total = rows * CHIPS
    once = pl.Buffered(1)
    full = pl.BlockSpec((rows, width), lambda i, c: (0, 0), pipeline_mode=once)
    return pl.pallas_call(
        functools.partial(middle_kernel, blk),
        grid_spec=pltpu.PrefetchScalarGridSpec(
            num_scalar_prefetch=1,
            grid=(9,),
            in_specs=[full] * 8
            + [
                pl.BlockSpec((1, total, LANES), lambda i, c: (8, 0, 0), pipeline_mode=once),
                pl.BlockSpec((2, total, LANES), lambda i, c: (jnp.clip(i - 1, 0, 3), 0, 0)),
                pl.BlockSpec((2, total, LANES), lambda i, c: (jnp.clip(i - 5, 0, 3), 0, 0)),
            ],
            out_specs=pl.BlockSpec((total, width), lambda i, c: (0, 0), pipeline_mode=once),
        ),
        out_shape=jax.ShapeDtypeStruct((total, width), BF16),
        compiler_params=params(),
        cost_estimate=cost(35),
        name="middle",
    )(chip, *parts, *mates, first_w, first_w, second_w)


def core_kernel(blk, chip_ref, *refs):
    own, mate, wts, outs = refs[0:4], refs[4:8], refs[8:12], refs[12:16]
    for rel in range(CHIPS):
        for pair in range(own[rel].shape[0] // (2 * blk)):
            at, nxt = pair * 2 * blk, pair * 2 * blk + blk
            z = jnp.concatenate(
                [own[rel][at:nxt, :], mate[rel][at:nxt, :], own[rel][nxt : nxt + blk, :], mate[rel][nxt : nxt + blk, :]], axis=0
            )
            outs[rel][at : at + 2 * blk, :] = mxu(wts[rel][0, at : at + 2 * blk, :], z).astype(BF16)


def core_stage(chip, own, mate, core_w, blk):
    total, width = own.shape
    rows = total // CHIPS
    tile = rows // 8

    def rel_spec(rel):
        return pl.BlockSpec((tile, width), lambda i, c: (((c[0] + rel) % CHIPS) * 8 + i, 0))

    def w_spec(rel):
        return pl.BlockSpec((1, tile, LANES), lambda i, c: (8, ((c[0] + rel) % CHIPS) * 8 + i, 0))

    data = [rel_spec(r) for r in range(CHIPS)]
    return pl.pallas_call(
        functools.partial(core_kernel, blk),
        grid_spec=pltpu.PrefetchScalarGridSpec(
            num_scalar_prefetch=1,
            grid=(8,),
            in_specs=data + data + [w_spec(r) for r in range(CHIPS)],
            out_specs=[pl.BlockSpec((tile, width), lambda i, c: (i, 0))] * 4,
        ),
        out_shape=[jax.ShapeDtypeStruct((rows, width), BF16)] * 4,
        compiler_params=params(),
        cost_estimate=cost(8),
        name="core_stage",
    )(chip, *[own] * 4, *[mate] * 4, *[core_w] * 4)


def solution(mesh):
    members = mesh.shape["sp"]
    groups = mesh.shape["dp"]

    def to_chip(value, shift):
        pairs = [(d, (d + shift * CORES) % members) for d in range(members)]
        return lax.ppermute(value, "sp", pairs)

    def to_core(value):
        return lax.ppermute(value, "sp", [(d, d ^ 1) for d in range(members)])

    def swap(parts):
        got = [parts[0]] + [None] * (CHIPS - 1)
        for shift in (2, 1, 3):
            got[-shift % CHIPS] = to_chip(parts[shift], shift)
        return got

    def device_program(signal, w_first, w_second):
        stages, _, _, blk, _ = w_first.shape
        rows, channels = signal.shape
        group = rows // CHIPS
        width = 256
        chunks = channels // width
        chip = lax.axis_index("sp") // CORES
        odd = chip % 2
        side = lax.axis_index("dp") % 2
        chip_arr = jnp.full((1,), chip, jnp.int32)

        def quarter(array, rel, col, wide, half=None):
            start = ((chip + rel) % CHIPS) * group
            if half is None:
                return lax.dynamic_slice(array, (start, col), (group, wide))
            return lax.dynamic_slice(array, (start + half * (group // 2), col), (group // 2, wide))

        def chip_weights(weights, hi, lo):
            packed = pack_pair(weights, hi, lo)
            if groups % 2:
                got = swap([quarter(packed, r, 0, LANES) for r in range(CHIPS)])
            else:
                own = quarter(packed, 0, 0, LANES)
                mine = swap([own] + [quarter(packed, r, 0, LANES, side) for r in range(1, CHIPS)])[1:]
            if groups % 2 == 0:
                theirs = [lax.ppermute(m, "dp", [(g, g ^ 1) for g in range(groups)]) for m in mine]
                both = [(jnp.where(side == 0, m, t), jnp.where(side == 0, t, m)) for m, t in zip(mine, theirs)]
                got = [own] + [jnp.concatenate(b, axis=0) for b in both]
            return expand_pair(got, odd, blk)

        w_first, w_second = (jnp.transpose(w, (0, 2, 3, 4, 1)) for w in (w_first, w_second))
        hi_first, lo_first = chip_weights(w_first, 0, 1)
        mid_first = spread(w_first, True)
        mid_second = spread(w_second, False)
        hi_second, lo_second = chip_weights(w_second, stages - 1, stages - 2)

        result = jnp.zeros((rows, channels), BF16)
        for c in range(chunks):
            parts = [quarter(signal, r, c * width, width) for r in range(CHIPS)]
            signal, parts = lax.optimization_barrier((signal, parts))
            parts = swap(parts)
            parts = chip_stages(parts, hi_first, lo_first, blk)
            parts = swap(parts)
            mates = [to_core(p) for p in parts]
            act = middle(chip_arr, parts, mates, mid_first, mid_second, blk)
            twin = to_core(act)
            parts = core_stage(chip_arr, act, twin, mid_second, blk)
            parts = swap(parts)
            parts = chip_stages(parts, lo_second, hi_second, blk)
            parts = swap(parts)
            for r in range(CHIPS):
                at = (((chip + r) % CHIPS) * group, c * width)
                result = lax.dynamic_update_slice(result, parts[r], at)
        return result

    row_spec = P(("dp", "sp"), None)
    weight_spec = P(None, "sp", None, None, None)
    return jax.shard_map(device_program, mesh=mesh, in_specs=(row_spec, weight_spec, weight_spec), out_specs=row_spec, check_vma=False)
```

```python
import functools

import jax
import jax.numpy as jnp
from jax import lax
from jax.experimental import pallas as pl
from jax.experimental.pallas import tpu as pltpu
from jax.sharding import PartitionSpec as P


CORES = 2
CHIPS = 4
LANES = 128
PAD = 8
BF16 = jnp.bfloat16
F32 = jnp.float32


def mxu(lhs, rhs):
    return jnp.dot(lhs, rhs, preferred_element_type=F32)


def cost(us):
    return pl.CostEstimate(flops=int(us * 1e8), bytes_accessed=int(us * 1e5), transcendentals=0)


def params():
    return pltpu.CompilerParams(dimension_semantics=("arbitrary",), vmem_limit_bytes=60 * 2**20)


def turned(refs, i, sel):
    wide = jnp.concatenate([ref[0, slot, i] for ref in refs for slot in range(2)], axis=0)
    return lax.dot_general(wide, sel, (((0,), (0,)), ((), ())), preferred_element_type=F32)


def unpad(tmp, out, pitch, blk):
    @pl.loop(0, tmp.shape[0] // (pitch * 8))
    def _(it):
        for u in range(8):
            b = it * 8 + u
            src = pl.ds(pl.multiple_of(b * pitch, 8), blk)
            out[pl.ds(pl.multiple_of(b * blk, blk), blk), :] = tmp[src, :].astype(BF16)


def pack_kernel(a_ref, b_ref, out_ref, tmp):
    blk, blocks = a_ref.shape[2], a_ref.shape[4]
    row = lax.broadcasted_iota(jnp.int32, (LANES, LANES), 0)
    col = lax.broadcasted_iota(jnp.int32, (LANES, LANES), 1)
    sel = (row == col).astype(F32).astype(BF16)

    @pl.loop(0, blk // 4)
    def _(it):
        for u in range(4):
            i = it * 4 + u
            tmp[pl.ds(i, blocks, stride=blk + PAD), :] = turned((a_ref, b_ref), i, sel)

    unpad(tmp, out_ref, blk + PAD, blk)


def pack_pair(turned_w, hi, lo):
    _, two, blk, _, blocks = turned_w.shape
    spec = lambda stage: pl.BlockSpec((1, two, blk, blk, blocks), lambda i: (stage, 0, 0, 0, 0))
    return pl.pallas_call(
        pack_kernel,
        grid=(1,),
        in_specs=[spec(hi), spec(lo)],
        out_specs=pl.BlockSpec((blocks * blk, LANES), lambda i: (0, 0)),
        out_shape=jax.ShapeDtypeStruct((blocks * blk, LANES), BF16),
        scratch_shapes=[pltpu.VMEM((blocks * (blk + PAD), LANES), F32)],
        compiler_params=params(),
        cost_estimate=cost(5),
        name="pack_pair",
    )(turned_w, turned_w)


def expand_kernel(d0, d1, d2, d3, sel_hi, sel_lo, out_hi, out_lo):
    for rel, src in enumerate((d0, d1, d2, d3)):
        val = src[...]
        out_hi[rel] = mxu(val, sel_hi[rel]).astype(BF16)
        out_lo[rel] = mxu(val, sel_lo[rel]).astype(BF16)


def expand_pair(packed, odd, blk):
    rows = packed[0].shape[0]
    tile = rows // 8
    shape = (CHIPS, LANES, LANES)
    rel, k, n = (lax.broadcasted_iota(jnp.int32, shape, axis) for axis in range(3))
    same = k % blk == n % blk
    kg, ng = k // blk, n // blk
    mate_lo = jnp.where(odd == 1, 3 - rel, rel ^ 1)
    sel_hi = (same & (((kg == 0) & (ng == rel)) | ((kg == 1) & (ng == (rel ^ 2))))).astype(BF16)
    sel_lo = (same & (((kg == 2) & (ng == rel)) | ((kg == 3) & (ng == mate_lo)))).astype(BF16)
    out = jax.ShapeDtypeStruct((CHIPS, rows, LANES), BF16)
    sel_spec = pl.BlockSpec(shape, lambda i: (0, 0, 0))
    out_spec = pl.BlockSpec((CHIPS, tile, LANES), lambda i: (0, i, 0))
    return pl.pallas_call(
        expand_kernel,
        grid=(rows // tile,),
        in_specs=[pl.BlockSpec((tile, LANES), lambda i: (i, 0))] * 4 + [sel_spec] * 2,
        out_specs=[out_spec] * 2,
        out_shape=[out] * 2,
        compiler_params=params(),
        cost_estimate=cost(5),
        name="expand_pair",
    )(*packed, sel_hi, sel_lo)


def spread_kernel(first_map, a_ref, b_ref, out_ref, tmp_a, tmp_b):
    step = pl.program_id(0)
    blk, blocks = a_ref.shape[2], a_ref.shape[4]
    lone = step == 4
    lo = jnp.where(lone, 0, 6 - 2 * step if first_map else 2 * step)
    row = lax.broadcasted_iota(jnp.int32, (LANES, 4 * LANES), 0)
    col = lax.broadcasted_iota(jnp.int32, (LANES, 4 * LANES), 1)
    fits = row % blk == col % blk
    sel = (fits & (row // blk == col // LANES)).astype(F32).astype(BF16)
    block = lax.broadcasted_iota(jnp.int32, (blocks, LANES), 0)
    group = lax.broadcasted_iota(jnp.int32, (blocks, LANES), 1) // blk
    own = jnp.where(lone, 2 * (block & 1), (block >> lo) & 3)
    first, second = (2, 1) if first_map else (1, 2)
    mates = [jnp.where(lone, own + 1, own ^ first), jnp.where(lone, own + 1, own ^ second)]

    @pl.loop(0, blk // 8)
    def _(it):
        wides = [turned((a_ref, b_ref), it * 8 + u, sel) for u in range(8)]
        for u, wide in enumerate(wides):
            for half, (mate, tmp) in enumerate(zip(mates, (tmp_a, tmp_b))):
                both = wide[:, 2 * half * LANES : 2 * (half + 1) * LANES]
                val = jnp.where(group == own, both[:, :LANES], jnp.where(group == mate, both[:, LANES:], 0.0))
                tmp[pl.ds(it * 8 + u, blocks, stride=blk + PAD), :] = val

    unpad(tmp_a, out_ref.at[0], blk + PAD, blk)
    unpad(tmp_b, out_ref.at[1], blk + PAD, blk)


def spread(turned_w, first_map):
    stages, two, blk, _, blocks = turned_w.shape
    if first_map:
        a_at = lambda i: jnp.where(i < 4, 3 + 2 * i, 2)
        b_at = lambda i: jnp.where(i < 4, 4 + 2 * i, 2)
    else:
        a_at = lambda i: 2 * i
        b_at = lambda i: jnp.minimum(2 * i + 1, stages - 3)
    spec = lambda at: pl.BlockSpec((1, two, blk, blk, blocks), lambda i: (at(i), 0, 0, 0, 0))
    rows = blocks * blk
    return pl.pallas_call(
        functools.partial(spread_kernel, first_map),
        grid=(5,),
        in_specs=[spec(a_at), spec(b_at)],
        out_specs=pl.BlockSpec((2, rows, LANES), lambda i: (i, 0, 0)),
        out_shape=jax.ShapeDtypeStruct((10, rows, LANES), BF16),
        scratch_shapes=[pltpu.VMEM((blocks * (blk + PAD), LANES), F32)] * 2,
        compiler_params=params(),
        cost_estimate=cost(25),
        name="spread",
    )(turned_w, turned_w)


def two_stages(quads):
    mids = [mxu(lhs_a, rows).astype(BF16) for lhs_a, _, rows in quads]
    return [mxu(lhs_b, mid).astype(BF16) for (_, lhs_b, _), mid in zip(quads, mids)]


def chip_kernel(blk, x0, x1, x2, x3, ea, eb, o0, o1, o2, o3):
    spans = [slice(b * blk, (b + 1) * blk) for b in range(x0.shape[0] // blk)]
    quads = []
    for rows in spans:
        z = jnp.concatenate([x[rows, :] for x in (x0, x1, x2, x3)], axis=0)
        a_mat = jnp.concatenate([ea[r, rows, :] for r in range(CHIPS)], axis=0)
        b_mat = jnp.concatenate([eb[r, rows, :] for r in range(CHIPS)], axis=0)
        quads.append((a_mat, b_mat, z))
    for rows, y in zip(spans, two_stages(quads)):
        for r, o in enumerate((o0, o1, o2, o3)):
            o[rows, :] = y[r * blk : (r + 1) * blk]


def chip_stages(parts, ea, eb, blk):
    rows, width = parts[0].shape
    tile = rows // 8
    spec = pl.BlockSpec((tile, width), lambda i: (i, 0))
    wspec = pl.BlockSpec((CHIPS, tile, LANES), lambda i: (0, i, 0))
    return pl.pallas_call(
        functools.partial(chip_kernel, blk),
        grid=(rows // tile,),
        in_specs=[spec] * 4 + [wspec] * 2,
        out_specs=[spec] * 4,
        out_shape=[jax.ShapeDtypeStruct((rows, width), BF16)] * 4,
        compiler_params=params(),
        cost_estimate=cost(8),
        name="chip_stages",
    )(*parts, ea, eb)


def gelu(x):
    x = x.astype(F32)
    return (0.5 * x * (1.0 + lax.erf(x * 0.7071067811865476))).astype(BF16)


def middle_kernel(blk, chip_ref, x0, x1, x2, x3, p0, p1, p2, p3, core_w, first_w, second_w, buf):
    step = pl.program_id(0)
    group_rows = x0.shape[0]
    unroll = 8

    @pl.when(step == 0)
    def _():
        for rel, (own, mate) in enumerate(zip((x0, x1, x2, x3), (p0, p1, p2, p3))):
            base = ((chip_ref[0] + rel) % CHIPS) * group_rows

            @pl.loop(0, group_rows // (2 * blk * unroll))
            def _(it):
                outs = []
                for u in range(unroll):
                    off = pl.multiple_of((it * unroll + u) * 2 * blk, 2 * blk)
                    nxt = pl.multiple_of(off + blk, blk)
                    dst = pl.multiple_of(base + off, 2 * blk)
                    z = jnp.concatenate(
                        [own[pl.ds(off, blk), :], mate[pl.ds(off, blk), :], own[pl.ds(nxt, blk), :], mate[pl.ds(nxt, blk), :]], axis=0
                    )
                    outs.append((dst, mxu(core_w[0, pl.ds(dst, 2 * blk), :], z).astype(BF16)))
                for dst, val in outs:
                    buf[pl.ds(dst, 2 * blk), :] = val

    def quad_step(wts, lo):
        @pl.loop(0, buf.shape[0] // (4 * blk * unroll))
        def _(it):
            places, quads = [], []
            for u in range(unroll):
                quad = it * unroll + u
                first = ((quad >> lo) << (lo + 2)) | (quad & ((1 << lo) - 1))
                offs = [pl.multiple_of((first + (pos << lo)) * blk, blk) for pos in range(4)]
                z = jnp.concatenate([buf[pl.ds(o, blk), :] for o in offs], axis=0)
                a_mat = jnp.concatenate([wts[0, pl.ds(o, blk), :] for o in offs], axis=0)
                b_mat = jnp.concatenate([wts[1, pl.ds(o, blk), :] for o in offs], axis=0)
                places.append(offs)
                quads.append((a_mat, b_mat, z))
            for offs, y in zip(places, two_stages(quads)):
                for pos, o in enumerate(offs):
                    buf[pl.ds(o, blk), :] = y[pos * blk : (pos + 1) * blk]

    @pl.when((step > 0) & (step <= 4))
    def _():
        quad_step(first_w, 8 - 2 * step)

    @pl.when(step == 4)
    def _():
        rows = 64

        @pl.loop(0, buf.shape[0] // rows)
        def _(it):
            at = pl.ds(pl.multiple_of(it * rows, rows), rows)
            buf[at, :] = gelu(buf[at, :])

    @pl.when(step > 4)
    def _():
        quad_step(second_w, 2 * step - 10)


def middle(chip, parts, mates, first_w, second_w, blk):
    rows, width = parts[0].shape
    total = rows * CHIPS
    once = pl.Buffered(1)
    full = pl.BlockSpec((rows, width), lambda i, c: (0, 0), pipeline_mode=once)
    return pl.pallas_call(
        functools.partial(middle_kernel, blk),
        grid_spec=pltpu.PrefetchScalarGridSpec(
            num_scalar_prefetch=1,
            grid=(9,),
            in_specs=[full] * 8
            + [
                pl.BlockSpec((1, total, LANES), lambda i, c: (8, 0, 0), pipeline_mode=once),
                pl.BlockSpec((2, total, LANES), lambda i, c: (jnp.clip(i - 1, 0, 3), 0, 0)),
                pl.BlockSpec((2, total, LANES), lambda i, c: (jnp.clip(i - 5, 0, 3), 0, 0)),
            ],
            out_specs=pl.BlockSpec((total, width), lambda i, c: (0, 0), pipeline_mode=once),
        ),
        out_shape=jax.ShapeDtypeStruct((total, width), BF16),
        compiler_params=params(),
        cost_estimate=cost(35),
        name="middle",
    )(chip, *parts, *mates, first_w, first_w, second_w)


def core_kernel(blk, chip_ref, *refs):
    own, mate, wts, outs = refs[0:4], refs[4:8], refs[8:12], refs[12:16]
    for rel in range(CHIPS):
        for pair in range(own[rel].shape[0] // (2 * blk)):
            at, nxt = pair * 2 * blk, pair * 2 * blk + blk
            z = jnp.concatenate(
                [own[rel][at:nxt, :], mate[rel][at:nxt, :], own[rel][nxt : nxt + blk, :], mate[rel][nxt : nxt + blk, :]], axis=0
            )
            outs[rel][at : at + 2 * blk, :] = mxu(wts[rel][0, at : at + 2 * blk, :], z).astype(BF16)


def core_stage(chip, own, mate, core_w, blk):
    total, width = own.shape
    rows = total // CHIPS
    tile = rows // 8

    def rel_spec(rel):
        return pl.BlockSpec((tile, width), lambda i, c: (((c[0] + rel) % CHIPS) * 8 + i, 0))

    def w_spec(rel):
        return pl.BlockSpec((1, tile, LANES), lambda i, c: (8, ((c[0] + rel) % CHIPS) * 8 + i, 0))

    data = [rel_spec(r) for r in range(CHIPS)]
    return pl.pallas_call(
        functools.partial(core_kernel, blk),
        grid_spec=pltpu.PrefetchScalarGridSpec(
            num_scalar_prefetch=1,
            grid=(8,),
            in_specs=data + data + [w_spec(r) for r in range(CHIPS)],
            out_specs=[pl.BlockSpec((tile, width), lambda i, c: (i, 0))] * 4,
        ),
        out_shape=[jax.ShapeDtypeStruct((rows, width), BF16)] * 4,
        compiler_params=params(),
        cost_estimate=cost(8),
        name="core_stage",
    )(chip, *[own] * 4, *[mate] * 4, *[core_w] * 4)


def solution(mesh):
    members = mesh.shape["sp"]
    groups = mesh.shape["dp"]

    def to_chip(value, shift):
        pairs = [(d, (d + shift * CORES) % members) for d in range(members)]
        return lax.ppermute(value, "sp", pairs)

    def to_core(value):
        return lax.ppermute(value, "sp", [(d, d ^ 1) for d in range(members)])

    def swap(parts):
        got = [parts[0]] + [None] * (CHIPS - 1)
        for shift in (2, 1, 3):
            got[-shift % CHIPS] = to_chip(parts[shift], shift)
        return got

    def device_program(signal, w_first, w_second):
        stages, _, _, blk, _ = w_first.shape
        rows, channels = signal.shape
        group = rows // CHIPS
        width = 256
        chunks = channels // width
        chip = lax.axis_index("sp") // CORES
        odd = chip % 2
        side = lax.axis_index("dp") % 2
        chip_arr = jnp.full((1,), chip, jnp.int32)

        def quarter(array, rel, col, wide, half=None):
            start = ((chip + rel) % CHIPS) * group
            if half is None:
                return lax.dynamic_slice(array, (start, col), (group, wide))
            return lax.dynamic_slice(array, (start + half * (group // 2), col), (group // 2, wide))

        def chip_weights(weights, hi, lo):
            packed = pack_pair(weights, hi, lo)
            if groups % 2:
                got = swap([quarter(packed, r, 0, LANES) for r in range(CHIPS)])
            else:
                own = quarter(packed, 0, 0, LANES)
                mine = swap([own] + [quarter(packed, r, 0, LANES, side) for r in range(1, CHIPS)])[1:]
            if groups % 2 == 0:
                theirs = [lax.ppermute(m, "dp", [(g, g ^ 1) for g in range(groups)]) for m in mine]
                both = [(jnp.where(side == 0, m, t), jnp.where(side == 0, t, m)) for m, t in zip(mine, theirs)]
                got = [own] + [jnp.concatenate(b, axis=0) for b in both]
            return expand_pair(got, odd, blk)

        w_first, w_second = (jnp.transpose(w, (0, 2, 3, 4, 1)) for w in (w_first, w_second))
        hi_first, lo_first = chip_weights(w_first, 0, 1)
        mid_first = spread(w_first, True)
        mid_second = spread(w_second, False)
        hi_second, lo_second = chip_weights(w_second, stages - 1, stages - 2)

        result = jnp.zeros((rows, channels), BF16)
        for c in range(chunks):
            far = quarter(signal, 2, c * width, width)
            signal, far = lax.optimization_barrier((signal, far))
            far = to_chip(far, 2)
            parts = [quarter(signal, r, c * width, width) for r in (0, 1, 3)]
            signal, parts = lax.optimization_barrier((signal, parts))
            parts = [parts[0], to_chip(parts[2], 3), far, to_chip(parts[1], 1)]
            parts = chip_stages(parts, hi_first, lo_first, blk)
            parts = swap(parts)
            mates = [to_core(p) for p in parts]
            act = middle(chip_arr, parts, mates, mid_first, mid_second, blk)
            twin = to_core(act)
            parts = core_stage(chip_arr, act, twin, mid_second, blk)
            parts = swap(parts)
            parts = chip_stages(parts, lo_second, hi_second, blk)
            parts = swap(parts)
            for r in range(CHIPS):
                at = (((chip + r) % CHIPS) * group, c * width)
                result = lax.dynamic_update_slice(result, parts[r], at)
        return result

    row_spec = P(("dp", "sp"), None)
    weight_spec = P(None, "sp", None, None, None)
    return jax.shard_map(device_program, mesh=mesh, in_specs=(row_spec, weight_spec, weight_spec), out_specs=row_spec, check_vma=False)
```

```python
import functools

import jax
import jax.numpy as jnp
from jax import lax
from jax.experimental import pallas as pl
from jax.experimental.pallas import tpu as pltpu
from jax.sharding import PartitionSpec as P


CORES = 2
CHIPS = 4
LANES = 128
PAD = 8
BF16 = jnp.bfloat16
F32 = jnp.float32


def mxu(lhs, rhs):
    return jnp.dot(lhs, rhs, preferred_element_type=F32)


def cost(us):
    return pl.CostEstimate(flops=int(us * 1e8), bytes_accessed=int(us * 1e5), transcendentals=0)


def params():
    return pltpu.CompilerParams(dimension_semantics=("arbitrary",), vmem_limit_bytes=60 * 2**20)


def turned(refs, i, sel):
    wide = jnp.concatenate([ref[0, slot, i] for ref in refs for slot in range(2)], axis=0)
    return lax.dot_general(wide, sel, (((0,), (0,)), ((), ())), preferred_element_type=F32)


def unpad(tmp, out, pitch, blk):
    @pl.loop(0, tmp.shape[0] // (pitch * 8))
    def _(it):
        for u in range(8):
            b = it * 8 + u
            src = pl.ds(pl.multiple_of(b * pitch, 8), blk)
            out[pl.ds(pl.multiple_of(b * blk, blk), blk), :] = tmp[src, :].astype(BF16)


def pack_kernel(a_ref, b_ref, out_ref, tmp):
    blk, blocks = a_ref.shape[2], a_ref.shape[4]
    row = lax.broadcasted_iota(jnp.int32, (LANES, LANES), 0)
    col = lax.broadcasted_iota(jnp.int32, (LANES, LANES), 1)
    sel = (row == col).astype(F32).astype(BF16)

    @pl.loop(0, blk // 4)
    def _(it):
        for u in range(4):
            i = it * 4 + u
            tmp[pl.ds(i, blocks, stride=blk + PAD), :] = turned((a_ref, b_ref), i, sel)

    unpad(tmp, out_ref, blk + PAD, blk)


def pack_pair(turned_w, hi, lo):
    _, two, blk, _, blocks = turned_w.shape
    spec = lambda stage: pl.BlockSpec((1, two, blk, blk, blocks), lambda i: (stage, 0, 0, 0, 0))
    return pl.pallas_call(
        pack_kernel,
        grid=(1,),
        in_specs=[spec(hi), spec(lo)],
        out_specs=pl.BlockSpec((blocks * blk, LANES), lambda i: (0, 0)),
        out_shape=jax.ShapeDtypeStruct((blocks * blk, LANES), BF16),
        scratch_shapes=[pltpu.VMEM((blocks * (blk + PAD), LANES), F32)],
        compiler_params=params(),
        cost_estimate=cost(5),
        name="pack_pair",
    )(turned_w, turned_w)


def expand_kernel(d0, d1, d2, d3, sel_hi, sel_lo, out_hi, out_lo):
    for rel, src in enumerate((d0, d1, d2, d3)):
        val = src[...]
        out_hi[rel] = mxu(val, sel_hi[rel]).astype(BF16)
        out_lo[rel] = mxu(val, sel_lo[rel]).astype(BF16)


def expand_pair(packed, odd, blk):
    rows = packed[0].shape[0]
    tile = rows // 8
    shape = (CHIPS, LANES, LANES)
    rel, k, n = (lax.broadcasted_iota(jnp.int32, shape, axis) for axis in range(3))
    same = k % blk == n % blk
    kg, ng = k // blk, n // blk
    mate_lo = jnp.where(odd == 1, 3 - rel, rel ^ 1)
    sel_hi = (same & (((kg == 0) & (ng == rel)) | ((kg == 1) & (ng == (rel ^ 2))))).astype(BF16)
    sel_lo = (same & (((kg == 2) & (ng == rel)) | ((kg == 3) & (ng == mate_lo)))).astype(BF16)
    out = jax.ShapeDtypeStruct((CHIPS, rows, LANES), BF16)
    sel_spec = pl.BlockSpec(shape, lambda i: (0, 0, 0))
    out_spec = pl.BlockSpec((CHIPS, tile, LANES), lambda i: (0, i, 0))
    return pl.pallas_call(
        expand_kernel,
        grid=(rows // tile,),
        in_specs=[pl.BlockSpec((tile, LANES), lambda i: (i, 0))] * 4 + [sel_spec] * 2,
        out_specs=[out_spec] * 2,
        out_shape=[out] * 2,
        compiler_params=params(),
        cost_estimate=cost(5),
        name="expand_pair",
    )(*packed, sel_hi, sel_lo)


def spread_kernel(first_map, a_ref, b_ref, out_ref, tmp_a, tmp_b):
    step = pl.program_id(0)
    blk, blocks = a_ref.shape[2], a_ref.shape[4]
    lone = step == 4
    lo = jnp.where(lone, 0, 6 - 2 * step if first_map else 2 * step)
    row = lax.broadcasted_iota(jnp.int32, (LANES, 4 * LANES), 0)
    col = lax.broadcasted_iota(jnp.int32, (LANES, 4 * LANES), 1)
    fits = row % blk == col % blk
    sel = (fits & (row // blk == col // LANES)).astype(F32).astype(BF16)
    block = lax.broadcasted_iota(jnp.int32, (blocks, LANES), 0)
    group = lax.broadcasted_iota(jnp.int32, (blocks, LANES), 1) // blk
    own = jnp.where(lone, 2 * (block & 1), (block >> lo) & 3)
    first, second = (2, 1) if first_map else (1, 2)
    mates = [jnp.where(lone, own + 1, own ^ first), jnp.where(lone, own + 1, own ^ second)]

    @pl.loop(0, blk // 8)
    def _(it):
        wides = [turned((a_ref, b_ref), it * 8 + u, sel) for u in range(8)]
        for u, wide in enumerate(wides):
            for half, (mate, tmp) in enumerate(zip(mates, (tmp_a, tmp_b))):
                both = wide[:, 2 * half * LANES : 2 * (half + 1) * LANES]
                val = jnp.where(group == own, both[:, :LANES], jnp.where(group == mate, both[:, LANES:], 0.0))
                tmp[pl.ds(it * 8 + u, blocks, stride=blk + PAD), :] = val

    unpad(tmp_a, out_ref.at[0], blk + PAD, blk)
    unpad(tmp_b, out_ref.at[1], blk + PAD, blk)


def spread(turned_w, first_map):
    stages, two, blk, _, blocks = turned_w.shape
    if first_map:
        a_at = lambda i: jnp.where(i < 4, 3 + 2 * i, 2)
        b_at = lambda i: jnp.where(i < 4, 4 + 2 * i, 2)
    else:
        a_at = lambda i: 2 * i
        b_at = lambda i: jnp.minimum(2 * i + 1, stages - 3)
    spec = lambda at: pl.BlockSpec((1, two, blk, blk, blocks), lambda i: (at(i), 0, 0, 0, 0))
    rows = blocks * blk
    return pl.pallas_call(
        functools.partial(spread_kernel, first_map),
        grid=(5,),
        in_specs=[spec(a_at), spec(b_at)],
        out_specs=pl.BlockSpec((2, rows, LANES), lambda i: (i, 0, 0)),
        out_shape=jax.ShapeDtypeStruct((10, rows, LANES), BF16),
        scratch_shapes=[pltpu.VMEM((blocks * (blk + PAD), LANES), F32)] * 2,
        compiler_params=params(),
        cost_estimate=cost(25),
        name="spread",
    )(turned_w, turned_w)


def two_stages(quads):
    mids = [mxu(lhs_a, rows).astype(BF16) for lhs_a, _, rows in quads]
    return [mxu(lhs_b, mid).astype(BF16) for (_, lhs_b, _), mid in zip(quads, mids)]


def chip_kernel(blk, x0, x1, x2, x3, ea, eb, o0, o1, o2, o3):
    spans = [slice(b * blk, (b + 1) * blk) for b in range(x0.shape[0] // blk)]
    quads = []
    for rows in spans:
        z = jnp.concatenate([x[rows, :] for x in (x0, x1, x2, x3)], axis=0)
        a_mat = jnp.concatenate([ea[r, rows, :] for r in range(CHIPS)], axis=0)
        b_mat = jnp.concatenate([eb[r, rows, :] for r in range(CHIPS)], axis=0)
        quads.append((a_mat, b_mat, z))
    for rows, y in zip(spans, two_stages(quads)):
        for r, o in enumerate((o0, o1, o2, o3)):
            o[rows, :] = y[r * blk : (r + 1) * blk]


def chip_stages(parts, ea, eb, blk):
    rows, width = parts[0].shape
    tile = rows // 4
    spec = pl.BlockSpec((tile, width), lambda i: (i, 0))
    wspec = pl.BlockSpec((CHIPS, tile, LANES), lambda i: (0, i, 0))
    return pl.pallas_call(
        functools.partial(chip_kernel, blk),
        grid=(rows // tile,),
        in_specs=[spec] * 4 + [wspec] * 2,
        out_specs=[spec] * 4,
        out_shape=[jax.ShapeDtypeStruct((rows, width), BF16)] * 4,
        compiler_params=params(),
        cost_estimate=cost(8),
        name="chip_stages",
    )(*parts, ea, eb)


def gelu(x):
    x = x.astype(F32)
    return (0.5 * x * (1.0 + lax.erf(x * 0.7071067811865476))).astype(BF16)


def middle_kernel(blk, chip_ref, x0, x1, x2, x3, p0, p1, p2, p3, core_w, first_w, second_w, buf):
    step = pl.program_id(0)
    group_rows = x0.shape[0]
    unroll = 16

    @pl.when(step == 0)
    def _():
        for rel, (own, mate) in enumerate(zip((x0, x1, x2, x3), (p0, p1, p2, p3))):
            base = ((chip_ref[0] + rel) % CHIPS) * group_rows

            @pl.loop(0, group_rows // (2 * blk * unroll))
            def _(it):
                outs = []
                for u in range(unroll):
                    off = pl.multiple_of((it * unroll + u) * 2 * blk, 2 * blk)
                    nxt = pl.multiple_of(off + blk, blk)
                    dst = pl.multiple_of(base + off, 2 * blk)
                    z = jnp.concatenate(
                        [own[pl.ds(off, blk), :], mate[pl.ds(off, blk), :], own[pl.ds(nxt, blk), :], mate[pl.ds(nxt, blk), :]], axis=0
                    )
                    outs.append((dst, mxu(core_w[0, pl.ds(dst, 2 * blk), :], z).astype(BF16)))
                for dst, val in outs:
                    buf[pl.ds(dst, 2 * blk), :] = val

    def quad_step(wts, lo):
        @pl.loop(0, buf.shape[0] // (4 * blk * unroll))
        def _(it):
            places, quads = [], []
            for u in range(unroll):
                quad = it * unroll + u
                first = ((quad >> lo) << (lo + 2)) | (quad & ((1 << lo) - 1))
                offs = [pl.multiple_of((first + (pos << lo)) * blk, blk) for pos in range(4)]
                z = jnp.concatenate([buf[pl.ds(o, blk), :] for o in offs], axis=0)
                a_mat = jnp.concatenate([wts[0, pl.ds(o, blk), :] for o in offs], axis=0)
                b_mat = jnp.concatenate([wts[1, pl.ds(o, blk), :] for o in offs], axis=0)
                places.append(offs)
                quads.append((a_mat, b_mat, z))
            for offs, y in zip(places, two_stages(quads)):
                for pos, o in enumerate(offs):
                    buf[pl.ds(o, blk), :] = y[pos * blk : (pos + 1) * blk]

    @pl.when((step > 0) & (step <= 4))
    def _():
        quad_step(first_w, 8 - 2 * step)

    @pl.when(step == 4)
    def _():
        rows = 64

        @pl.loop(0, buf.shape[0] // rows)
        def _(it):
            at = pl.ds(pl.multiple_of(it * rows, rows), rows)
            buf[at, :] = gelu(buf[at, :])

    @pl.when(step > 4)
    def _():
        quad_step(second_w, 2 * step - 10)


def middle(chip, parts, mates, first_w, second_w, blk):
    rows, width = parts[0].shape
    total = rows * CHIPS
    once = pl.Buffered(1)
    full = pl.BlockSpec((rows, width), lambda i, c: (0, 0), pipeline_mode=once)
    return pl.pallas_call(
        functools.partial(middle_kernel, blk),
        grid_spec=pltpu.PrefetchScalarGridSpec(
            num_scalar_prefetch=1,
            grid=(9,),
            in_specs=[full] * 8
            + [
                pl.BlockSpec((1, total, LANES), lambda i, c: (8, 0, 0), pipeline_mode=once),
                pl.BlockSpec((2, total, LANES), lambda i, c: (jnp.clip(i - 1, 0, 3), 0, 0)),
                pl.BlockSpec((2, total, LANES), lambda i, c: (jnp.clip(i - 5, 0, 3), 0, 0)),
            ],
            out_specs=pl.BlockSpec((total, width), lambda i, c: (0, 0), pipeline_mode=once),
        ),
        out_shape=jax.ShapeDtypeStruct((total, width), BF16),
        compiler_params=params(),
        cost_estimate=cost(35),
        name="middle",
    )(chip, *parts, *mates, first_w, first_w, second_w)


def core_kernel(blk, chip_ref, *refs):
    own, mate, wts, outs = refs[0:4], refs[4:8], refs[8:12], refs[12:16]
    for rel in range(CHIPS):
        for pair in range(own[rel].shape[0] // (2 * blk)):
            at, nxt = pair * 2 * blk, pair * 2 * blk + blk
            z = jnp.concatenate(
                [own[rel][at:nxt, :], mate[rel][at:nxt, :], own[rel][nxt : nxt + blk, :], mate[rel][nxt : nxt + blk, :]], axis=0
            )
            outs[rel][at : at + 2 * blk, :] = mxu(wts[rel][0, at : at + 2 * blk, :], z).astype(BF16)


def core_stage(chip, own, mate, core_w, blk):
    total, width = own.shape
    rows = total // CHIPS
    tile = rows // 8

    def rel_spec(rel):
        return pl.BlockSpec((tile, width), lambda i, c: (((c[0] + rel) % CHIPS) * 8 + i, 0))

    def w_spec(rel):
        return pl.BlockSpec((1, tile, LANES), lambda i, c: (8, ((c[0] + rel) % CHIPS) * 8 + i, 0))

    data = [rel_spec(r) for r in range(CHIPS)]
    return pl.pallas_call(
        functools.partial(core_kernel, blk),
        grid_spec=pltpu.PrefetchScalarGridSpec(
            num_scalar_prefetch=1,
            grid=(8,),
            in_specs=data + data + [w_spec(r) for r in range(CHIPS)],
            out_specs=[pl.BlockSpec((tile, width), lambda i, c: (i, 0))] * 4,
        ),
        out_shape=[jax.ShapeDtypeStruct((rows, width), BF16)] * 4,
        compiler_params=params(),
        cost_estimate=cost(8),
        name="core_stage",
    )(chip, *[own] * 4, *[mate] * 4, *[core_w] * 4)


def solution(mesh):
    members = mesh.shape["sp"]
    groups = mesh.shape["dp"]

    def to_chip(value, shift):
        pairs = [(d, (d + shift * CORES) % members) for d in range(members)]
        return lax.ppermute(value, "sp", pairs)

    def to_core(value):
        return lax.ppermute(value, "sp", [(d, d ^ 1) for d in range(members)])

    def swap(parts):
        got = [parts[0]] + [None] * (CHIPS - 1)
        for shift in (2, 1, 3):
            got[-shift % CHIPS] = to_chip(parts[shift], shift)
        return got

    def device_program(signal, w_first, w_second):
        stages, _, _, blk, _ = w_first.shape
        rows, channels = signal.shape
        group = rows // CHIPS
        width = 256
        chunks = channels // width
        chip = lax.axis_index("sp") // CORES
        odd = chip % 2
        side = lax.axis_index("dp") % 2
        chip_arr = jnp.full((1,), chip, jnp.int32)

        def quarter(array, rel, col, wide, half=None):
            start = ((chip + rel) % CHIPS) * group
            if half is None:
                return lax.dynamic_slice(array, (start, col), (group, wide))
            return lax.dynamic_slice(array, (start + half * (group // 2), col), (group // 2, wide))

        def chip_weights(weights, hi, lo):
            packed = pack_pair(weights, hi, lo)
            if groups % 2:
                got = swap([quarter(packed, r, 0, LANES) for r in range(CHIPS)])
            else:
                own = quarter(packed, 0, 0, LANES)
                mine = swap([own] + [quarter(packed, r, 0, LANES, side) for r in range(1, CHIPS)])[1:]
            if groups % 2 == 0:
                theirs = [lax.ppermute(m, "dp", [(g, g ^ 1) for g in range(groups)]) for m in mine]
                both = [(jnp.where(side == 0, m, t), jnp.where(side == 0, t, m)) for m, t in zip(mine, theirs)]
                got = [own] + [jnp.concatenate(b, axis=0) for b in both]
            return expand_pair(got, odd, blk)

        w_first, w_second = (jnp.transpose(w, (0, 2, 3, 4, 1)) for w in (w_first, w_second))
        hi_first, lo_first = chip_weights(w_first, 0, 1)
        mid_first = spread(w_first, True)
        mid_second = spread(w_second, False)
        hi_second, lo_second = chip_weights(w_second, stages - 1, stages - 2)

        result = jnp.zeros((rows, channels), BF16)
        for c in range(chunks):
            far = quarter(signal, 2, c * width, width)
            signal, far = lax.optimization_barrier((signal, far))
            far = to_chip(far, 2)
            parts = [quarter(signal, r, c * width, width) for r in (0, 1, 3)]
            signal, parts = lax.optimization_barrier((signal, parts))
            parts = [parts[0], to_chip(parts[2], 3), far, to_chip(parts[1], 1)]
            parts = chip_stages(parts, hi_first, lo_first, blk)
            parts = swap(parts)
            mates = [to_core(p) for p in parts]
            act = middle(chip_arr, parts, mates, mid_first, mid_second, blk)
            twin = to_core(act)
            parts = core_stage(chip_arr, act, twin, mid_second, blk)
            parts = swap(parts)
            parts = chip_stages(parts, lo_second, hi_second, blk)
            far = parts[2]
            cuts = 1 if c + 1 < chunks else 2
            size = group // cuts
            far = [to_chip(far[i * size : (i + 1) * size], 2) for i in range(cuts)]
            pieces = [(0, 0, parts[0]), (3, 0, to_chip(parts[1], 1)), (1, 0, to_chip(parts[3], 3))]
            pieces += [(2, i * size, piece) for i, piece in enumerate(far)]
            for r, row, piece in pieces:
                at = (((chip + r) % CHIPS) * group + row, c * width)
                result = lax.dynamic_update_slice(result, piece, at)
        return result

    row_spec = P(("dp", "sp"), None)
    weight_spec = P(None, "sp", None, None, None)
    return jax.shard_map(device_program, mesh=mesh, in_specs=(row_spec, weight_spec, weight_spec), out_specs=row_spec, check_vma=False)
```

```python
import functools

import jax
import jax.numpy as jnp
from jax import lax
from jax.experimental import pallas as pl
from jax.experimental.pallas import tpu as pltpu
from jax.sharding import PartitionSpec as P


CORES = 2
CHIPS = 4
LANES = 128
PAD = 8
BF16 = jnp.bfloat16
F32 = jnp.float32


def mxu(lhs, rhs):
    return jnp.dot(lhs, rhs, preferred_element_type=F32)


def cost(us):
    return pl.CostEstimate(flops=int(us * 1e8), bytes_accessed=int(us * 1e5), transcendentals=0)


def params():
    return pltpu.CompilerParams(dimension_semantics=("arbitrary",), vmem_limit_bytes=60 * 2**20)


def turned(refs, i, sel):
    wide = jnp.concatenate([ref[0, slot, i] for ref in refs for slot in range(2)], axis=0)
    return lax.dot_general(wide, sel, (((0,), (0,)), ((), ())), preferred_element_type=F32)


def unpad(tmp, out, pitch, blk):
    @pl.loop(0, tmp.shape[0] // (pitch * 8))
    def _(it):
        for u in range(8):
            b = it * 8 + u
            src = pl.ds(pl.multiple_of(b * pitch, 8), blk)
            out[pl.ds(pl.multiple_of(b * blk, blk), blk), :] = tmp[src, :].astype(BF16)


def pack_kernel(a_ref, b_ref, out_ref, tmp):
    blk, blocks = a_ref.shape[2], a_ref.shape[4]
    row = lax.broadcasted_iota(jnp.int32, (LANES, LANES), 0)
    col = lax.broadcasted_iota(jnp.int32, (LANES, LANES), 1)
    sel = (row == col).astype(F32).astype(BF16)

    @pl.loop(0, blk // 4)
    def _(it):
        for u in range(4):
            i = it * 4 + u
            tmp[pl.ds(i, blocks, stride=blk + PAD), :] = turned((a_ref, b_ref), i, sel)

    unpad(tmp, out_ref, blk + PAD, blk)


def pack_pair(turned_w, hi, lo):
    _, two, blk, _, blocks = turned_w.shape
    spec = lambda stage: pl.BlockSpec((1, two, blk, blk, blocks), lambda i: (stage, 0, 0, 0, 0))
    return pl.pallas_call(
        pack_kernel,
        grid=(1,),
        in_specs=[spec(hi), spec(lo)],
        out_specs=pl.BlockSpec((blocks * blk, LANES), lambda i: (0, 0)),
        out_shape=jax.ShapeDtypeStruct((blocks * blk, LANES), BF16),
        scratch_shapes=[pltpu.VMEM((blocks * (blk + PAD), LANES), F32)],
        compiler_params=params(),
        cost_estimate=cost(5),
        name="pack_pair",
    )(turned_w, turned_w)


def expand_kernel(d0, d1, d2, d3, sel_hi, sel_lo, out_hi, out_lo):
    for rel, src in enumerate((d0, d1, d2, d3)):
        val = src[...]
        out_hi[rel] = mxu(val, sel_hi[rel]).astype(BF16)
        out_lo[rel] = mxu(val, sel_lo[rel]).astype(BF16)


def expand_pair(packed, odd, blk):
    rows = packed[0].shape[0]
    tile = rows // 4
    shape = (CHIPS, LANES, LANES)
    rel, k, n = (lax.broadcasted_iota(jnp.int32, shape, axis) for axis in range(3))
    same = k % blk == n % blk
    kg, ng = k // blk, n // blk
    mate_lo = jnp.where(odd == 1, 3 - rel, rel ^ 1)
    sel_hi = (same & (((kg == 0) & (ng == rel)) | ((kg == 1) & (ng == (rel ^ 2))))).astype(BF16)
    sel_lo = (same & (((kg == 2) & (ng == rel)) | ((kg == 3) & (ng == mate_lo)))).astype(BF16)
    out = jax.ShapeDtypeStruct((CHIPS, rows, LANES), BF16)
    sel_spec = pl.BlockSpec(shape, lambda i: (0, 0, 0))
    out_spec = pl.BlockSpec((CHIPS, tile, LANES), lambda i: (0, i, 0))
    return pl.pallas_call(
        expand_kernel,
        grid=(rows // tile,),
        in_specs=[pl.BlockSpec((tile, LANES), lambda i: (i, 0))] * 4 + [sel_spec] * 2,
        out_specs=[out_spec] * 2,
        out_shape=[out] * 2,
        compiler_params=params(),
        cost_estimate=cost(5),
        name="expand_pair",
    )(*packed, sel_hi, sel_lo)


def spread_kernel(first_map, a_ref, b_ref, out_ref, tmp_a, tmp_b):
    step = pl.program_id(0)
    blk, blocks = a_ref.shape[2], a_ref.shape[4]
    lone = step == 4
    lo = jnp.where(lone, 0, 6 - 2 * step if first_map else 2 * step)
    row = lax.broadcasted_iota(jnp.int32, (LANES, 4 * LANES), 0)
    col = lax.broadcasted_iota(jnp.int32, (LANES, 4 * LANES), 1)
    fits = row % blk == col % blk
    sel = (fits & (row // blk == col // LANES)).astype(F32).astype(BF16)
    block = lax.broadcasted_iota(jnp.int32, (blocks, LANES), 0)
    group = lax.broadcasted_iota(jnp.int32, (blocks, LANES), 1) // blk
    own = jnp.where(lone, 2 * (block & 1), (block >> lo) & 3)
    first, second = (2, 1) if first_map else (1, 2)
    mates = [jnp.where(lone, own + 1, own ^ first), jnp.where(lone, own + 1, own ^ second)]

    @pl.loop(0, blk // 8)
    def _(it):
        wides = [turned((a_ref, b_ref), it * 8 + u, sel) for u in range(8)]
        for u, wide in enumerate(wides):
            for half, (mate, tmp) in enumerate(zip(mates, (tmp_a, tmp_b))):
                both = wide[:, 2 * half * LANES : 2 * (half + 1) * LANES]
                val = jnp.where(group == own, both[:, :LANES], jnp.where(group == mate, both[:, LANES:], 0.0))
                tmp[pl.ds(it * 8 + u, blocks, stride=blk + PAD), :] = val

    unpad(tmp_a, out_ref.at[0], blk + PAD, blk)
    unpad(tmp_b, out_ref.at[1], blk + PAD, blk)


def spread(turned_w, first_map):
    stages, two, blk, _, blocks = turned_w.shape
    if first_map:
        a_at = lambda i: jnp.where(i < 4, 3 + 2 * i, 2)
        b_at = lambda i: jnp.where(i < 4, 4 + 2 * i, 2)
    else:
        a_at = lambda i: 2 * i
        b_at = lambda i: jnp.minimum(2 * i + 1, stages - 3)
    spec = lambda at: pl.BlockSpec((1, two, blk, blk, blocks), lambda i: (at(i), 0, 0, 0, 0))
    rows = blocks * blk
    return pl.pallas_call(
        functools.partial(spread_kernel, first_map),
        grid=(5,),
        in_specs=[spec(a_at), spec(b_at)],
        out_specs=pl.BlockSpec((2, rows, LANES), lambda i: (i, 0, 0)),
        out_shape=jax.ShapeDtypeStruct((10, rows, LANES), BF16),
        scratch_shapes=[pltpu.VMEM((blocks * (blk + PAD), LANES), F32)] * 2,
        compiler_params=params(),
        cost_estimate=cost(25),
        name="spread",
    )(turned_w, turned_w)


def two_stages(quads):
    mids = [mxu(lhs_a, rows).astype(BF16) for lhs_a, _, rows in quads]
    return [mxu(lhs_b, mid).astype(BF16) for (_, lhs_b, _), mid in zip(quads, mids)]


def chip_kernel(blk, x0, x1, x2, x3, ea, eb, o0, o1, o2, o3):
    spans = [slice(b * blk, (b + 1) * blk) for b in range(x0.shape[0] // blk)]
    quads = []
    for rows in spans:
        z = jnp.concatenate([x[rows, :] for x in (x0, x1, x2, x3)], axis=0)
        a_mat = jnp.concatenate([ea[r, rows, :] for r in range(CHIPS)], axis=0)
        b_mat = jnp.concatenate([eb[r, rows, :] for r in range(CHIPS)], axis=0)
        quads.append((a_mat, b_mat, z))
    for rows, y in zip(spans, two_stages(quads)):
        for r, o in enumerate((o0, o1, o2, o3)):
            o[rows, :] = y[r * blk : (r + 1) * blk]


def chip_stages(parts, ea, eb, blk):
    rows, width = parts[0].shape
    tile = rows // 4
    spec = pl.BlockSpec((tile, width), lambda i: (i, 0))
    wspec = pl.BlockSpec((CHIPS, tile, LANES), lambda i: (0, i, 0))
    return pl.pallas_call(
        functools.partial(chip_kernel, blk),
        grid=(rows // tile,),
        in_specs=[spec] * 4 + [wspec] * 2,
        out_specs=[spec] * 4,
        out_shape=[jax.ShapeDtypeStruct((rows, width), BF16)] * 4,
        compiler_params=params(),
        cost_estimate=cost(8),
        name="chip_stages",
    )(*parts, ea, eb)


def gelu(x):
    x = x.astype(F32)
    return (0.5 * x * (1.0 + lax.erf(x * 0.7071067811865476))).astype(BF16)


def middle_kernel(blk, chip_ref, x0, x1, x2, x3, p0, p1, p2, p3, core_w, first_w, second_w, buf):
    step = pl.program_id(0)
    group_rows = x0.shape[0]
    unroll = 16

    @pl.when(step == 0)
    def _():
        for rel, (own, mate) in enumerate(zip((x0, x1, x2, x3), (p0, p1, p2, p3))):
            base = ((chip_ref[0] + rel) % CHIPS) * group_rows

            @pl.loop(0, group_rows // (2 * blk * unroll))
            def _(it):
                outs = []
                for u in range(unroll):
                    off = pl.multiple_of((it * unroll + u) * 2 * blk, 2 * blk)
                    nxt = pl.multiple_of(off + blk, blk)
                    dst = pl.multiple_of(base + off, 2 * blk)
                    z = jnp.concatenate(
                        [own[pl.ds(off, blk), :], mate[pl.ds(off, blk), :], own[pl.ds(nxt, blk), :], mate[pl.ds(nxt, blk), :]], axis=0
                    )
                    outs.append((dst, mxu(core_w[0, pl.ds(dst, 2 * blk), :], z).astype(BF16)))
                for dst, val in outs:
                    buf[pl.ds(dst, 2 * blk), :] = val

    def quad_step(wts, lo):
        @pl.loop(0, buf.shape[0] // (4 * blk * unroll))
        def _(it):
            places, quads = [], []
            for u in range(unroll):
                quad = it * unroll + u
                first = ((quad >> lo) << (lo + 2)) | (quad & ((1 << lo) - 1))
                offs = [pl.multiple_of((first + (pos << lo)) * blk, blk) for pos in range(4)]
                z = jnp.concatenate([buf[pl.ds(o, blk), :] for o in offs], axis=0)
                a_mat = jnp.concatenate([wts[0, pl.ds(o, blk), :] for o in offs], axis=0)
                b_mat = jnp.concatenate([wts[1, pl.ds(o, blk), :] for o in offs], axis=0)
                places.append(offs)
                quads.append((a_mat, b_mat, z))
            for offs, y in zip(places, two_stages(quads)):
                for pos, o in enumerate(offs):
                    buf[pl.ds(o, blk), :] = y[pos * blk : (pos + 1) * blk]

    @pl.when((step > 0) & (step <= 4))
    def _():
        quad_step(first_w, 8 - 2 * step)

    @pl.when(step == 4)
    def _():
        rows = 64

        @pl.loop(0, buf.shape[0] // rows)
        def _(it):
            at = pl.ds(pl.multiple_of(it * rows, rows), rows)
            buf[at, :] = gelu(buf[at, :])

    @pl.when(step > 4)
    def _():
        quad_step(second_w, 2 * step - 10)


def middle(chip, parts, mates, first_w, second_w, blk):
    rows, width = parts[0].shape
    total = rows * CHIPS
    once = pl.Buffered(1)
    full = pl.BlockSpec((rows, width), lambda i, c: (0, 0), pipeline_mode=once)
    return pl.pallas_call(
        functools.partial(middle_kernel, blk),
        grid_spec=pltpu.PrefetchScalarGridSpec(
            num_scalar_prefetch=1,
            grid=(9,),
            in_specs=[full] * 8
            + [
                pl.BlockSpec((1, total, LANES), lambda i, c: (8, 0, 0), pipeline_mode=once),
                pl.BlockSpec((2, total, LANES), lambda i, c: (jnp.clip(i - 1, 0, 3), 0, 0)),
                pl.BlockSpec((2, total, LANES), lambda i, c: (jnp.clip(i - 5, 0, 3), 0, 0)),
            ],
            out_specs=pl.BlockSpec((total, width), lambda i, c: (0, 0), pipeline_mode=once),
        ),
        out_shape=jax.ShapeDtypeStruct((total, width), BF16),
        compiler_params=params(),
        cost_estimate=cost(35),
        name="middle",
    )(chip, *parts, *mates, first_w, first_w, second_w)


def core_kernel(blk, chip_ref, *refs):
    own, mate, wts, outs = refs[0:4], refs[4:8], refs[8:12], refs[12:16]
    for rel in range(CHIPS):
        for pair in range(own[rel].shape[0] // (2 * blk)):
            at, nxt = pair * 2 * blk, pair * 2 * blk + blk
            z = jnp.concatenate(
                [own[rel][at:nxt, :], mate[rel][at:nxt, :], own[rel][nxt : nxt + blk, :], mate[rel][nxt : nxt + blk, :]], axis=0
            )
            outs[rel][at : at + 2 * blk, :] = mxu(wts[rel][0, at : at + 2 * blk, :], z).astype(BF16)


def core_stage(chip, own, mate, core_w, blk):
    total, width = own.shape
    rows = total // CHIPS
    steps = 4
    tile = rows // steps

    def rel_spec(rel):
        return pl.BlockSpec((tile, width), lambda i, c: (((c[0] + rel) % CHIPS) * steps + i, 0))

    def w_spec(rel):
        return pl.BlockSpec((1, tile, LANES), lambda i, c: (8, ((c[0] + rel) % CHIPS) * steps + i, 0))

    data = [rel_spec(r) for r in range(CHIPS)]
    return pl.pallas_call(
        functools.partial(core_kernel, blk),
        grid_spec=pltpu.PrefetchScalarGridSpec(
            num_scalar_prefetch=1,
            grid=(steps,),
            in_specs=data + data + [w_spec(r) for r in range(CHIPS)],
            out_specs=[pl.BlockSpec((tile, width), lambda i, c: (i, 0))] * 4,
        ),
        out_shape=[jax.ShapeDtypeStruct((rows, width), BF16)] * 4,
        compiler_params=params(),
        cost_estimate=cost(8),
        name="core_stage",
    )(chip, *[own] * 4, *[mate] * 4, *[core_w] * 4)


def solution(mesh):
    members = mesh.shape["sp"]
    groups = mesh.shape["dp"]

    def to_chip(value, shift):
        pairs = [(d, (d + shift * CORES) % members) for d in range(members)]
        return lax.ppermute(value, "sp", pairs)

    def to_core(value):
        return lax.ppermute(value, "sp", [(d, d ^ 1) for d in range(members)])

    def swap(parts):
        got = [parts[0]] + [None] * (CHIPS - 1)
        for shift in (2, 1, 3):
            got[-shift % CHIPS] = to_chip(parts[shift], shift)
        return got

    def device_program(signal, w_first, w_second):
        stages, _, _, blk, _ = w_first.shape
        rows, channels = signal.shape
        group = rows // CHIPS
        width = 256
        chunks = channels // width
        chip = lax.axis_index("sp") // CORES
        odd = chip % 2
        side = lax.axis_index("dp") % 2
        chip_arr = jnp.full((1,), chip, jnp.int32)

        def quarter(array, rel, col, wide, half=None):
            start = ((chip + rel) % CHIPS) * group
            if half is None:
                return lax.dynamic_slice(array, (start, col), (group, wide))
            return lax.dynamic_slice(array, (start + half * (group // 2), col), (group // 2, wide))

        def chip_weights(weights, hi, lo):
            packed = pack_pair(weights, hi, lo)
            if groups % 2:
                got = swap([quarter(packed, r, 0, LANES) for r in range(CHIPS)])
            else:
                own = quarter(packed, 0, 0, LANES)
                mine = swap([own] + [quarter(packed, r, 0, LANES, side) for r in range(1, CHIPS)])[1:]
            if groups % 2 == 0:
                theirs = [lax.ppermute(m, "dp", [(g, g ^ 1) for g in range(groups)]) for m in mine]
                both = [(jnp.where(side == 0, m, t), jnp.where(side == 0, t, m)) for m, t in zip(mine, theirs)]
                got = [own] + [jnp.concatenate(b, axis=0) for b in both]
            return expand_pair(got, odd, blk)

        w_first, w_second = (jnp.transpose(w, (0, 2, 3, 4, 1)) for w in (w_first, w_second))
        hi_first, lo_first = chip_weights(w_first, 0, 1)
        mid_first = spread(w_first, True)
        mid_second = spread(w_second, False)
        hi_second, lo_second = chip_weights(w_second, stages - 1, stages - 2)

        result = jnp.zeros((rows, channels), BF16)
        for c in range(chunks):
            far = quarter(signal, 2, c * width, width)
            signal, far = lax.optimization_barrier((signal, far))
            far = to_chip(far, 2)
            parts = [quarter(signal, r, c * width, width) for r in (0, 1, 3)]
            signal, parts = lax.optimization_barrier((signal, parts))
            parts = [parts[0], to_chip(parts[2], 3), far, to_chip(parts[1], 1)]
            parts = chip_stages(parts, hi_first, lo_first, blk)
            parts = swap(parts)
            mates = [to_core(p) for p in parts]
            act = middle(chip_arr, parts, mates, mid_first, mid_second, blk)
            twin = to_core(act)
            parts = core_stage(chip_arr, act, twin, mid_second, blk)
            parts = swap(parts)
            parts = chip_stages(parts, lo_second, hi_second, blk)
            far = parts[2]
            cuts = 1 if c + 1 < chunks else 2
            size = group // cuts
            far = [to_chip(far[i * size : (i + 1) * size], 2) for i in range(cuts)]
            pieces = [(0, 0, parts[0]), (3, 0, to_chip(parts[1], 1)), (1, 0, to_chip(parts[3], 3))]
            pieces += [(2, i * size, piece) for i, piece in enumerate(far)]
            for r, row, piece in pieces:
                at = (((chip + r) % CHIPS) * group + row, c * width)
                result = lax.dynamic_update_slice(result, piece, at)
        return result

    row_spec = P(("dp", "sp"), None)
    weight_spec = P(None, "sp", None, None, None)
    return jax.shard_map(device_program, mesh=mesh, in_specs=(row_spec, weight_spec, weight_spec), out_specs=row_spec, check_vma=False)
```
